32 devices in a mesh: pipe: 1, seq: 32 (over z, y, x, core).
Axes of the slice: x: 2, y: 2, z: 4, core: 2. Of those that a mesh axis runs over, the one named last changes fastest.
Arguments:
- previous: bfloat16 [1, 4096, 8192], P('pipe', 'seq'), may hold values from -6 to 6
- saved_head_inputs: bfloat16 [1, 4096, 8192], P('pipe', 'seq'), may hold values from -0.29882812 to 0.29882812
- input_b: bfloat16 [1, 4096, 1024], P('pipe', 'seq'), may hold values from -0.5 to 0.5
- input_c: bfloat16 [1, 4096, 1024], P('pipe', 'seq'), may hold values from -0.5 to 0.5
- steps: float32 [1, 4096, 128], P('pipe', 'seq'), may hold values from 0.1 to 6553.6, as said below
- decay_rate: float32 [1, 128], P('pipe'), may hold values from 6.1035156e-05 to 0.05
- skip_gain: float32 [1, 128], P('pipe'), may hold values from 0.5 to 1.5
- segment_ids: int32 [1, 4096], P('pipe', 'seq'), may hold values from 0 to 3, never falling along the last dimension, each value on 1 to 2048 neighbouring positions
- advantage_mask: int32 [4096], P('seq'), may hold values 0 or 1
Outputs:
- grad_x: bfloat16 [1, 4096, 8192], P('pipe', 'seq')
- grad_b: bfloat16 [1, 4096, 1024], P('pipe', 'seq')
- grad_c: bfloat16 [1, 4096, 1024], P('pipe', 'seq')
- bypass_gain_adjoint: float32 [1, 128], P('pipe')
The draws below stay inside these ranges and needn't reach their ends.
Inputs may be any that keep to these rules, and one draw needn't show every extreme that they name: `steps`: Positive; in a few positions of each section the step is 1.6 * 4096 for every head.
All inputs are finite; a program needn't handle non-finite values. No bound on the sum of `advantage_mask` on one device may be relied on, other than what follows from the above.
Results may differ from the reference program's by a relative error of at most 0.0095.
Values may be sent and summed in bfloat16 or wider, within the bound.
A program may use at most 128 MiB of HBM per device.

```python
import math
import jax
import jax.numpy as jnp
import numpy as np
from jax import lax

HEADS = 128
HEAD_DIM = 64
STATE = 128
GROUPS = 8
BLOCK = 256
TOK_DEV = 128
MERGED_POSITIONS = 4096
N_PIPE = 1
N_SEQ = 32


def draw_steps(key, part):
    first, second, tertiary_multiplier = jax.random.split(key, 3)
    starting_position = jax.random.uniform(first, (N_PIPE, MERGED_POSITIONS, HEADS), jnp.float32, 0.5, 2.0)
    factor = jax.random.uniform(second, (N_PIPE, MERGED_POSITIONS // TOK_DEV, 1, 1), jnp.float32, 1.0, 2.5)
    starting_position = (starting_position.reshape(N_PIPE, MERGED_POSITIONS // TOK_DEV, TOK_DEV, HEADS) * factor).reshape(N_PIPE, MERGED_POSITIONS, HEADS)
    relay_interval = jax.random.randint(tertiary_multiplier, (N_PIPE, MERGED_POSITIONS, 1), 0, max(MERGED_POSITIONS // 4, 1)) == 0
    return jnp.where(relay_interval, jnp.float32(1.6 * MERGED_POSITIONS), starting_position)


def with_ends(entries, stream_key, low, top_value):
    longest = entries.shape.index(max(entries.shape))
    spots = []
    for shift in (0, 1):
        where = [jax.random.randint(jax.random.fold_in(stream_key, axis), (), 0, length) for axis, length in enumerate(entries.shape)]
        where[longest] = (where[longest] + shift) % entries.shape[longest]
        spots.append(tuple(where))
    return entries.at[spots[0]].set(low).at[spots[1]].set(top_value)


def levels(key, shape, cuts, low, high):
    level = 1.0
    for position, shards_of in cuts:
        heights = jax.random.uniform(jax.random.fold_in(jax.random.fold_in(key, 6), position), (shards_of,), jnp.float32, low / len(cuts), high / len(cuts))
        level = level * jnp.repeat(jnp.exp(heights), shape[position] // shards_of).reshape((-1,) + (1,) * (len(shape) - 1 - position))
    return level


def length_profile(count, total, bound, slope):
    portions = [(1 << 20) // math.isqrt(standing ** slope) + 1 for standing in range(2, count + 1)]
    spare, holding = total - bound - (count - 1), [1] * (count - 1)
    while spare > 0:
        free = [i for i in range(count - 1) if holding[i] < bound]
        pool, left = sum([portions[i] for i in free]), spare
        for i in free:
            more = min(bound - holding[i], max(1, left * portions[i] // pool), spare)
            holding[i] = holding[i] + more
            spare = spare - more
    return np.array([bound] + holding)


def ragged(own_key, number_of, total, most, lean):
    if number_of == 2:
        one = jax.random.randint(own_key, (), max(1, total - most), min(most, total - 1) + 1)
        return jnp.stack([one, total - one])
    lengths = jnp.asarray(length_profile(number_of, total, most, lean), jnp.int32)
    pairs = (number_of - 1) // 2
    donor, sink = lengths[1:1 + 2 * pairs:2], lengths[2:2 + 2 * pairs:2]
    margin = jnp.minimum(donor - 1, most - sink)
    shifted = jax.random.randint(jax.random.fold_in(own_key, 1), (pairs,), 0, 1 << 20) % (margin + 1)
    lengths = lengths.at[1:1 + 2 * pairs:2].set(donor - shifted).at[2:2 + 2 * pairs:2].set(sink + shifted)
    return lengths[jax.random.permutation(jax.random.fold_in(own_key, 2), number_of)]


def scatter_about(key, dims, deviation, most, cuts=(), dtype=jnp.bfloat16):
    loudness = levels(key, dims, cuts, -0.22, 0.18) if cuts else 1.0
    result = jax.random.normal(key, dims, jnp.float32) * deviation * loudness
    return jnp.minimum(jnp.maximum(result, -most), most).astype(dtype)


def setup_inputs(seed: int = 0) -> dict:
    arg_keys = jax.random.split(jax.random.key(seed), 10)
    return {
        "previous": scatter_about(arg_keys[0], (N_PIPE, MERGED_POSITIONS, HEADS * HEAD_DIM), 1.0, 6.0, ((1, 32),)),
        "saved_head_inputs": scatter_about(arg_keys[1], (N_PIPE, MERGED_POSITIONS, HEADS * HEAD_DIM), 0.05, 0.29882812, ((1, 32),)),
        "input_b": scatter_about(arg_keys[2], (N_PIPE, MERGED_POSITIONS, GROUPS * STATE), STATE ** -0.5, 0.5, ((1, 32),)),
        "input_c": scatter_about(arg_keys[3], (N_PIPE, MERGED_POSITIONS, GROUPS * STATE), STATE ** -0.5, 0.5, ((1, 32),)),
        "steps": draw_steps(jax.random.fold_in(arg_keys[9], 71), 0),
        "decay_rate": jnp.clip(jnp.exp(jax.random.uniform(arg_keys[5], (N_PIPE, HEADS), jnp.float32, math.log(6.103515625e-05), math.log(0.05))), 6.103515625e-05, 0.05),
        "skip_gain": jnp.clip(1.0 + 0.1 * jax.random.normal(arg_keys[6], (N_PIPE, HEADS), jnp.float32), 0.5, 1.5),
        "segment_ids": jax.vmap(lambda own: jnp.searchsorted(jnp.cumsum(ragged(own, max(2, N_SEQ // 8), MERGED_POSITIONS, MERGED_POSITIONS // 2, 1)), jnp.arange(MERGED_POSITIONS), side="right"))(jax.random.split(arg_keys[7], N_PIPE)).reshape((N_PIPE, MERGED_POSITIONS)).astype(jnp.int32),
        "advantage_mask": with_ends((jax.random.randint(arg_keys[8], (MERGED_POSITIONS,), 0, 4) < 3).astype(jnp.int32), jax.random.fold_in(arg_keys[8], 1), 0, 1),
    }


def mix(form, left, right):
    return jnp.einsum(form, left.astype(jnp.float32), right.astype(jnp.float32))


def prepare(seg, prev, steps_here, rate):
    length = seg.shape[0]
    cum = jnp.cumsum(-steps_here * rate[None, :], axis=0)
    row = lax.broadcasted_iota(jnp.int32, (length, length), 0)
    col = lax.broadcasted_iota(jnp.int32, (length, length), 1)
    link = (seg[:, None] == seg[None, :]) & (row >= col)
    spread = cum[:, None, :] - cum[None, :, :]
    kernel = jnp.exp(jnp.where(link[:, :, None], spread, -1e30))
    enter = jnp.exp(cum) * (seg == prev)[:, None].astype(jnp.float32)
    leave = jnp.exp(cum[-1][None, :] - cum) * (seg == seg[-1])[:, None].astype(jnp.float32)
    through = jnp.exp(cum[-1]) * (seg[-1] == prev).astype(jnp.float32)
    return kernel, enter, leave, through


def block_states(grad4, inputs4, bmat, cmat, enter, leave):
    shape = grad4.shape
    xo = (leave.reshape(shape[0], shape[1], shape[2])[..., None] * inputs4).astype(jnp.bfloat16)
    gi = (enter.reshape(shape[0], shape[1], shape[2])[..., None] * grad4).astype(jnp.bfloat16)
    state = mix("tgkp,tgn->gkpn", xo, bmat)
    adjoint = mix("tgkp,tgn->gkpn", gi, cmat)
    return xo, gi, state, adjoint


def block_grads(grad4, inputs4, bmat, cmat, kernel, leave, xo, gi, entering_state, later, skip):
    length, groups, per_group, head_dim = grad4.shape
    kernel4 = kernel.reshape(length, length, groups, per_group)
    prod = mix("tgkp,ugkp->tugk", grad4, inputs4)
    w_one = (prod * kernel4).astype(jnp.bfloat16)
    cross = mix("tgn,ugn->tug", bmat, cmat)
    w_two = (jnp.swapaxes(kernel4, 0, 1) * cross[:, :, :, None]).astype(jnp.bfloat16)
    grad_c = mix("tugk,ugn->tgn", w_one, bmat) + mix("tgkp,gkpn->tgn", gi, entering_state)
    grad_b = mix("utgk,ugn->tgn", w_one, cmat) + mix("tgkp,gkpn->tgn", xo, later)
    leave4 = leave.reshape(length, groups, per_group)[..., None]
    grad_x = mix("tugk,ugkp->tgkp", w_two, grad4) + leave4 * mix("tgn,gkpn->tgkp", bmat, later)
    grad_x = grad_x + skip.reshape(groups, per_group)[None, :, :, None] * grad4.astype(jnp.float32)
    return grad_x, grad_b, grad_c


def section_backward(incoming, inputs_here, bmat_here, cmat_here, step_here, seg_here, rate, skip, groups, per_group):
    tokens = incoming.shape[0]
    heads = groups * per_group
    head_dim = incoming.shape[1] // heads
    blocks = tokens // BLOCK
    grads = incoming.reshape(blocks, BLOCK, groups, per_group, head_dim)
    inputs = inputs_here.reshape(blocks, BLOCK, groups, per_group, head_dim)
    bmats = bmat_here.reshape(blocks, BLOCK, groups, STATE)
    cmats = cmat_here.reshape(blocks, BLOCK, groups, STATE)
    segs = seg_here.reshape(blocks, BLOCK).astype(jnp.int32)
    prevs = jnp.concatenate([jnp.full((1,), -1, jnp.int32), segs[:-1, -1].astype(jnp.int32)])
    step_blocks = step_here.reshape(blocks, BLOCK, heads)

    def first_pass(item):
        seg, prev, steps_here, grad4, inputs4, bmat, cmat = item
        kernel, enter, leave, through = prepare(seg, prev, steps_here, rate)
        xo, gi, state, adjoint = block_states(grad4, inputs4, bmat, cmat, enter, leave)
        return through.reshape(groups, per_group), state, adjoint

    items = (segs, prevs, step_blocks, grads, inputs, bmats, cmats)
    through, states, adjoints = lax.map(first_pass, items)
    zeros = jnp.zeros((groups, per_group, head_dim, STATE), jnp.float32)

    def forward(carry, item):
        return carry * item[0][:, :, None, None] + item[1], carry

    def backward(carry, item):
        return item[1] + item[0][:, :, None, None] * carry, carry

    unused_one, entering_state = lax.scan(forward, zeros, (through, states))
    unused_two, later = lax.scan(backward, zeros, (through, adjoints), reverse=True)
    entering_state = entering_state.astype(jnp.bfloat16)
    later = later.astype(jnp.bfloat16)

    def second_pass(item):
        seg, prev, steps_here, grad4, inputs4, bmat, cmat, enter_state, later_state = item
        kernel, enter, leave, discarded_result = prepare(seg, prev, steps_here, rate)
        xo, gi, state, adjoint = block_states(grad4, inputs4, bmat, cmat, enter, leave)
        return block_grads(grad4, inputs4, bmat, cmat, kernel, leave, xo, gi, enter_state, later_state, skip)

    grad_x, grad_b, grad_c = lax.map(second_pass, items + (entering_state, later))
    return grad_x.reshape(tokens, heads * head_dim), grad_b.reshape(tokens, groups * STATE), grad_c.reshape(tokens, groups * STATE)


def reference(previous, saved_head_inputs, input_b, input_c, steps, decay_rate, skip_gain, segment_ids, advantage_mask):
    sections = previous.shape[0]
    tokens = previous.shape[1]
    heads = decay_rate.shape[1]
    head_dim = previous.shape[2] // heads
    groups = input_b.shape[2] // STATE
    per_group = heads // groups
    out_x, out_b, out_c, out_skip = [], [], [], []
    for section in range(sections):
        if section == sections - 1:
            incoming = previous[section] * advantage_mask.astype(jnp.bfloat16)[:, None]
        else:
            incoming = previous[section + 1]
        grad_x, grad_b, grad_c = section_backward(incoming, saved_head_inputs[section], input_b[section], input_c[section], steps[section], segment_ids[section], decay_rate[section], skip_gain[section], groups, per_group)
        out_x.append(grad_x.astype(jnp.bfloat16))
        out_b.append(grad_b.astype(jnp.bfloat16))
        out_c.append(grad_c.astype(jnp.bfloat16))
        out_skip.append(mix("thp,thp->h", incoming.reshape(tokens, heads, head_dim), saved_head_inputs[section].reshape(tokens, heads, head_dim)))
    return jnp.stack(out_x), jnp.stack(out_b), jnp.stack(out_c), jnp.stack(out_skip)
```

```python
import functools

import jax
import jax.numpy as jnp
from jax import lax
from jax.experimental import pallas as pl
from jax.experimental.pallas import tpu as pltpu
from jax.sharding import PartitionSpec as P

STATE = 128
F32 = jnp.float32
BF16 = jnp.bfloat16
NT = (((1,), (1,)), ((), ()))
TN = (((0,), (0,)), ((), ()))


def dot(left, right, dims=(((1,), (0,)), ((), ()))):
    return lax.dot_general(left, right, dims, preferred_element_type=F32)


def spread_heads(factor, group, members, head_dim):
    heads = factor.shape[1]
    width = members * head_dim
    row = lax.broadcasted_iota(jnp.int32, (heads, width), 0)
    col = lax.broadcasted_iota(jnp.int32, (heads, width), 1)
    pick = (row == group * members + col // head_dim).astype(F32).astype(BF16)
    high = factor.astype(BF16)
    low = (factor - high.astype(F32)).astype(BF16)
    return dot(high, pick) + dot(low, pick)


def states_kernel(members, head_dim, prev, xin, bmat, cmat, leave, enter, mask, state, adjoint, skip_part):
    group = pl.program_id(0)
    grad = prev[...].astype(F32) * mask[...]
    x = xin[...].astype(F32)
    skip_part[0] = jnp.sum(grad * x, axis=0, keepdims=True)
    xo = (spread_heads(leave[...], group, members, head_dim) * x).astype(BF16)
    gi = (spread_heads(enter[...], group, members, head_dim) * grad).astype(BF16)
    state[0] = dot(bmat[...], xo, TN).astype(BF16)
    adjoint[0] = dot(cmat[...], gi, TN).astype(BF16)


def local_kernel(
    members, head_dim, prev, xin, bmat, cmat, cum, cum_rows, seg_col, seg_row, mask, grad_x, grad_b, grad_c
):
    length = prev.shape[0]
    row = lax.broadcasted_iota(jnp.int32, (length, length), 0)
    col = lax.broadcasted_iota(jnp.int32, (length, length), 1)
    link = (seg_col[...] == seg_row[...]) & (col >= row)
    bias = jnp.where(link, 0.0, -1e30).astype(F32)
    b = bmat[...]
    c = cmat[...]
    cross = dot(b, c, NT)
    grad = (prev[...].astype(F32) * mask[...]).astype(BF16)
    cums = cum[0]
    total = jnp.zeros((length, length), F32)
    for head in range(members):
        lanes = slice(head * head_dim, (head + 1) * head_dim)
        g = grad[:, lanes]
        x = xin[:, lanes]
        decay = jnp.exp(jnp.where(link, cum_rows[head : head + 1, :] - cums[:, head : head + 1], bias))
        total = total + decay * dot(x, g, NT)
        grad_x[:, lanes] = dot((decay * cross).astype(BF16), g)
    total = total.astype(BF16)
    grad_b[...] = dot(total, c)
    grad_c[...] = dot(total, b, TN)


def final_kernel(
    members, head_dim, prev, xin, bmat, leave, enter, mask, skip, near_x, near_b, near_c, entering, later,
    grad_x, grad_b, grad_c
):
    group = pl.program_id(0)
    grad = prev[...].astype(F32) * mask[...]
    x = xin[...].astype(F32)
    left = spread_heads(leave[...], group, members, head_dim)
    xo = (left * x).astype(BF16)
    gi = (spread_heads(enter[...], group, members, head_dim) * grad).astype(BF16)
    after = later[0]
    grad_x[...] = (near_x[...] + left * dot(bmat[...], after) + skip[...] * grad).astype(BF16)
    grad_b[...] = (near_b[...] + dot(xo, after, NT)).astype(BF16)
    grad_c[...] = (near_c[...] + dot(gi, entering[0], NT)).astype(BF16)


def shifted(value, steps):
    count = lax.axis_size("seq")
    initial, last = (max(0, -steps), min(count, count - steps))
    return lax.ppermute(value, "seq", [(s, s + steps) for s in range(initial, last)])


def swapped(value, level):
    count = lax.axis_size("seq")
    return lax.ppermute(value, "seq", [(s, s ^ 1 << level) for s in range(count)])


def on_device(
    previous, saved_head_inputs, input_b, input_c, steps, decay_rate, skip_gain, segment_ids, advantage_mask
):
    mask = advantage_mask.astype(F32)
    source = previous[0]
    sections = lax.axis_size("pipe")
    if sections > 1:
        last = lax.axis_index("pipe") == sections - 1
        arrived = lax.ppermute(previous, "pipe", [(s, s - 1) for s in range(1, sections)])[0]
        source = jnp.where(last, source, arrived)
        mask = jnp.where(last, mask, 1.0)
    mask = mask[:, None]
    x, bmat, cmat = saved_head_inputs[0], input_b[0], input_c[0]
    length = source.shape[0]
    heads = decay_rate.shape[1]
    head_dim = source.shape[1] // heads
    groups = bmat.shape[1] // STATE
    members = heads // groups
    width = members * head_dim
    devices = lax.axis_size("seq")
    place = lax.axis_index("seq")
    seg = segment_ids[0]

    lower = jnp.tril(jnp.ones((length, length), F32))
    cum = jnp.dot(lower, -steps[0] * decay_rate, precision=lax.Precision.HIGHEST)
    enter = jnp.exp(cum) * (seg == seg[0])[:, None]
    leave = jnp.exp(cum[-1:] - cum) * (seg == seg[-1])[:, None]

    token_wide = pl.BlockSpec((length, width), lambda g: (0, g))
    token_state = pl.BlockSpec((length, STATE), lambda g: (0, g))
    factor = pl.BlockSpec((length, heads), lambda g: (0, 0))
    column = pl.BlockSpec((length, 1), lambda g: (0, 0))
    slot = pl.BlockSpec((1, STATE, width), lambda g: (g, 0, 0))
    params = pltpu.CompilerParams(dimension_semantics=("arbitrary",), vmem_limit_bytes=60 << 20)

    state, adjoint, skip_part = pl.pallas_call(
        functools.partial(states_kernel, members, head_dim),
        grid=(groups,),
        in_specs=[token_wide, token_wide, token_state, token_state, factor, factor, column],
        out_specs=[slot, slot, pl.BlockSpec((1, 1, width), lambda g: (g, 0, 0))],
        out_shape=[
            jax.ShapeDtypeStruct((groups, STATE, width), BF16),
            jax.ShapeDtypeStruct((groups, STATE, width), BF16),
            jax.ShapeDtypeStruct((groups, 1, width), F32),
        ],
        compiler_params=params,
        name="block_states",
    )(source, x, bmat, cmat, leave, enter, mask)

    near_x, near_b, near_c = pl.pallas_call(
        functools.partial(local_kernel, members, head_dim),
        grid=(groups,),
        in_specs=[
            token_wide, token_wide, token_state, token_state,
            pl.BlockSpec((1, length, members), lambda g: (g, 0, 0)),
            pl.BlockSpec((members, length), lambda g: (g, 0)),
            column,
            pl.BlockSpec((1, length), lambda g: (0, 0)),
            column,
        ],
        out_specs=[token_wide, token_state, token_state],
        out_shape=[
            jax.ShapeDtypeStruct((length, heads * head_dim), F32),
            jax.ShapeDtypeStruct((length, groups * STATE), F32),
            jax.ShapeDtypeStruct((length, groups * STATE), F32),
        ],
        compiler_params=params,
        name="within_block",
    )(
        source, x, bmat, cmat,
        jnp.swapaxes(cum.reshape(length, groups, members), 0, 1), cum.T, seg[:, None], seg[None, :], mask,
    )

    skip_sum = jnp.sum(skip_part.reshape(heads, head_dim), axis=1)
    ends = jnp.pad(jnp.stack([seg[0], seg[-1]]).astype(F32), (0, heads - 2))
    table = lax.all_gather(jnp.stack([cum[-1], ends]), "seq", axis=0)
    bypass_gain_adjoint = lax.psum(skip_sum, "seq")
    first, final = table[:, 1, 0], table[:, 1, 1]
    behind = jnp.concatenate([jnp.full((1,), -1.0, F32), final[:-1]])
    links = (first == behind).astype(F32)
    through = jnp.exp(table[:, 0]) * (links * (first == final))[:, None]
    own_link = lax.dynamic_index_in_dim(links, place, 0, keepdims=False)

    levels = groups.bit_length() - 1
    pieces = devices // groups
    rows = []
    for level in range(levels):
        spans = jnp.prod(through.reshape(devices >> level, 1 << level, heads), axis=1)
        low = (place >> level) & ~1
        rows.append(lax.dynamic_slice_in_dim(spans, low, 2, 0))
    per_piece = jnp.prod(through.reshape(pieces, groups, heads), axis=1)
    padded = jnp.pad(per_piece, ((pieces, pieces), (0, 0)), constant_values=1.0)
    rows.append(lax.dynamic_slice_in_dim(padded, place // groups, 2 * pieces + 1, 0))
    rows = jnp.concatenate(rows, axis=0)
    rows = jnp.repeat(rows, head_dim, axis=1).reshape(-1, groups, 1, width)

    fwd = state
    bwd = (adjoint.astype(F32) * own_link).astype(BF16)
    kept = []
    for level in range(levels):
        half = fwd.shape[0] // 2
        right = (place >> level & 1) == 1
        mine = jnp.where(right, half, 0)

        def keep(value):
            return lax.dynamic_slice_in_dim(value, mine, half, 0)

        def give(value):
            return lax.dynamic_slice_in_dim(value, half - mine, half, 0)

        fwd_other = swapped(give(fwd), level)
        bwd_other = swapped(give(bwd), level)
        fwd_own, bwd_own = keep(fwd), keep(bwd)
        rows = lax.dynamic_slice_in_dim(rows, mine, half, 1)
        decay_left, decay_right = rows[2 * level], rows[2 * level + 1]
        fwd_left = jnp.where(right, fwd_other, fwd_own)
        fwd_right = jnp.where(right, fwd_own, fwd_other)
        bwd_left = jnp.where(right, bwd_other, bwd_own)
        bwd_right = jnp.where(right, bwd_own, bwd_other)
        kept.append((right, mine, half, fwd_left, bwd_right, decay_left, decay_right))
        fwd = (fwd_right.astype(F32) + decay_right * fwd_left.astype(F32)).astype(BF16)
        bwd = (bwd_left.astype(F32) + decay_left * bwd_right.astype(F32)).astype(BF16)

    across = rows[2 * levels :]
    entering = jnp.zeros(fwd.shape, F32)
    later = jnp.zeros(bwd.shape, F32)
    factor_in = factor_out = jnp.ones(across.shape[1:], F32)
    for distance in range(1, pieces):
        entering = entering + factor_in * shifted(fwd, distance * groups).astype(F32)
        later = later + factor_out * shifted(bwd, -distance * groups).astype(F32)
        factor_in = factor_in * across[pieces - distance]
        factor_out = factor_out * across[pieces + distance]

    for level in reversed(range(levels)):
        right, mine, half, fwd_left, bwd_right, decay_left, decay_right = kept[level]
        in_right = (fwd_left.astype(F32) + decay_left * entering).astype(BF16)
        out_left = (bwd_right.astype(F32) + decay_right * later).astype(BF16)
        in_left, out_right = entering.astype(BF16), later.astype(BF16)
        got_in = swapped(jnp.where(right, in_left, in_right), level)
        got_out = swapped(jnp.where(right, out_left, out_right), level)
        own_in = jnp.where(right, in_right, in_left)
        own_out = jnp.where(right, out_right, out_left)

        def join(own, got):
            return jnp.concatenate([jnp.where(right, got, own), jnp.where(right, own, got)], axis=0)

        entering = join(own_in, got_in)
        later = join(own_out, got_out)
        if level:
            entering, later = entering.astype(F32), later.astype(F32)

    grad_x, grad_b, grad_c = pl.pallas_call(
        functools.partial(final_kernel, members, head_dim),
        grid=(groups,),
        in_specs=[
            token_wide, token_wide, token_state, factor, factor, column,
            pl.BlockSpec((1, width), lambda g: (0, g)),
            token_wide, token_state, token_state, slot, slot,
        ],
        out_specs=[token_wide, token_state, token_state],
        out_shape=[
            jax.ShapeDtypeStruct((length, heads * head_dim), BF16),
            jax.ShapeDtypeStruct((length, groups * STATE), BF16),
            jax.ShapeDtypeStruct((length, groups * STATE), BF16),
        ],
        compiler_params=params,
        name="across_blocks",
    )(
        source, x, bmat, leave, enter * own_link, mask, jnp.repeat(skip_gain, head_dim, axis=1),
        near_x, near_b, near_c, entering, later,
    )
    return grad_x[None], grad_b[None], grad_c[None], bypass_gain_adjoint[None]


def solution(mesh):
    return jax.shard_map(
        on_device,
        mesh=mesh,
        in_specs=(
            P("pipe", "seq", None),
            P("pipe", "seq", None),
            P("pipe", "seq", None),
            P("pipe", "seq", None),
            P("pipe", "seq", None),
            P("pipe", None),
            P("pipe", None),
            P("pipe", "seq"),
            P("seq"),
        ),
        out_specs=(
            P("pipe", "seq", None),
            P("pipe", "seq", None),
            P("pipe", "seq", None),
            P("pipe", None),
        ),
        check_vma=False,
    )
```
